32 devices in a mesh: dp: 1 (over z), col: 4 (over y), row: 8 (over x, core).
Axes of the slice: x: 4, y: 4, z: 1, core: 2. Of those that a mesh axis runs over, the one named last changes fastest.
The devices are a block of a 4x4x8 slice.
Arguments:
- x_in: bfloat16 [8, 2048, 1536], P(('dp', 'row'), None, 'col')
- ln1_scale: float32 [1536], P('col')
- ln1_shift: float32 [1536], P('col')
- w_qkv: bfloat16 [1536, 4608], P('row', 'col')
- b_qkv: float32 [16, 288], P('col')
- w_o: bfloat16 [1536, 1536], P('row', 'col')
- b_o: float32 [1536], P('col')
- ln2_scale: float32 [1536], P('col')
- ln2_shift: float32 [1536], P('col')
- w_in: bfloat16 [1536, 6144], P('row', 'col')
- b_in: float32 [6144], P('col')
- w_out: bfloat16 [6144, 1536], P('row', 'col')
- b_out: float32 [1536], P('col')
- grad_out: bfloat16 [8, 2048, 1536], P(('dp', 'row'), None, 'col')
Outputs:
- output 1: bfloat16 [8, 2048, 1536], P(('dp', 'row'), None, 'col')
- output 2: bfloat16 [8, 2048, 1536], P(('dp', 'row'), None, 'col')
- output 3: float32 [1536], P(('dp', 'col'))
- output 4: float32 [1536], P(('dp', 'col'))
- output 5: bfloat16 [1536, 4608], P(('dp', 'row'), 'col')
- output 6: float32 [16, 288], P(('dp', 'col'))
- output 7: bfloat16 [1536, 1536], P(('dp', 'row'), 'col')
- output 8: float32 [1536], P(('dp', 'col'))
- output 9: float32 [1536], P(('dp', 'col'))
- output 10: float32 [1536], P(('dp', 'col'))
- output 11: bfloat16 [1536, 6144], P(('dp', 'row'), 'col')
- output 12: float32 [6144], P(('dp', 'col'))
- output 13: bfloat16 [6144, 1536], P(('dp', 'row'), 'col')
- output 14: float32 [1536], P(('dp', 'col'))
All inputs are finite; a program needn't handle non-finite values.
Results may differ from the reference program's by a relative error of at most 0.0112138.
Values are sent between devices in bfloat16 or wider.
A program may use at most 768 MiB of HBM per device.

```python
import jax
import jax.numpy as jnp
from jax import lax

BATCH = 8
SEQ_LEN = 2048
D_MODEL = 1536
NUM_HEADS = 16
HEAD_DIM = 96
D_FF = 6144
LN_EPS = 1e-5


def setup_inputs(seed: int = 0, part: int = 0) -> dict:
    shared = jax.random.split(jax.random.key(seed), 12)
    part_keys = jax.random.split(jax.random.fold_in(jax.random.key(seed + 1), part), 3)

    def draw_normal(key_in, arr_shape, spread):
        return jax.random.normal(key_in, arr_shape, jnp.float32) * spread

    act_shape = (BATCH, SEQ_LEN, D_MODEL)
    feat_mean = draw_normal(part_keys[0], (D_MODEL,), 1.0)
    x_in = (draw_normal(part_keys[1], act_shape, 1.0) + feat_mean).astype(jnp.bfloat16)
    return {
        'x_in': x_in,
        'ln1_scale': 1.0 + draw_normal(shared[0], (D_MODEL,), 0.3),
        'ln1_shift': draw_normal(shared[1], (D_MODEL,), 0.3),
        'w_qkv': draw_normal(shared[2], (D_MODEL, 3 * D_MODEL), D_MODEL ** -0.5).astype(jnp.bfloat16),
        'b_qkv': draw_normal(shared[3], (NUM_HEADS, 3 * HEAD_DIM), 0.5),
        'w_o': draw_normal(shared[4], (D_MODEL, D_MODEL), D_MODEL ** -0.5).astype(jnp.bfloat16),
        'b_o': draw_normal(shared[5], (D_MODEL,), 0.5),
        'ln2_scale': 1.0 + draw_normal(shared[6], (D_MODEL,), 0.3),
        'ln2_shift': draw_normal(shared[7], (D_MODEL,), 0.3),
        'w_in': draw_normal(shared[8], (D_MODEL, D_FF), D_MODEL ** -0.5).astype(jnp.bfloat16),
        'b_in': draw_normal(shared[9], (D_FF,), 0.5),
        'w_out': draw_normal(shared[10], (D_FF, D_MODEL), D_FF ** -0.5).astype(jnp.bfloat16),
        'b_out': draw_normal(shared[11], (D_MODEL,), 0.5),
        'grad_out': draw_normal(part_keys[2], act_shape, 1.0).astype(jnp.bfloat16),
    }


def layer_norm(act_in, ln_scale, ln_shift):
    act_f32 = act_in.astype(jnp.float32)
    mean_val = jnp.mean(act_f32, axis=-1, keepdims=True)
    variance = jnp.mean(act_f32 * act_f32, axis=-1, keepdims=True) - mean_val * mean_val
    return ((act_f32 - mean_val) * lax.rsqrt(variance + LN_EPS) * ln_scale + ln_shift).astype(jnp.bfloat16)


def attend_one(head_item):
    scores = jnp.dot(head_item[0], head_item[1].T, preferred_element_type=jnp.float32) * HEAD_DIM ** -0.5
    query_pos = lax.broadcasted_iota(jnp.int32, (SEQ_LEN, SEQ_LEN), 0)
    key_pos = lax.broadcasted_iota(jnp.int32, (SEQ_LEN, SEQ_LEN), 1)
    attn_probs = jax.nn.softmax(jnp.where(key_pos <= query_pos, scores, -1e30), axis=-1)
    return jnp.dot(attn_probs.astype(jnp.bfloat16), head_item[2], preferred_element_type=jnp.float32).astype(jnp.bfloat16)


def layer_forward(x_in, ln1_scale, ln1_shift, w_qkv, b_qkv, w_o, b_o, ln2_scale, ln2_shift, w_in, b_in, w_out, b_out):
    tokens = BATCH * SEQ_LEN
    x_rows = x_in.reshape(tokens, D_MODEL)
    normed1 = layer_norm(x_rows, ln1_scale, ln1_shift)
    qkv_rows = (jnp.dot(normed1, w_qkv, preferred_element_type=jnp.float32) + b_qkv.reshape(3 * D_MODEL)).astype(jnp.bfloat16)
    head_items = qkv_rows.reshape(BATCH, SEQ_LEN, NUM_HEADS, 3, HEAD_DIM).transpose(0, 2, 3, 1, 4)
    head_items = head_items.reshape(BATCH * NUM_HEADS, 3, SEQ_LEN, HEAD_DIM)
    attn_items = lax.map(jax.checkpoint(attend_one), head_items)
    attn_rows = attn_items.reshape(BATCH, NUM_HEADS, SEQ_LEN, HEAD_DIM).transpose(0, 2, 1, 3).reshape(tokens, D_MODEL)
    resid_rows = (x_rows.astype(jnp.float32) + jnp.dot(attn_rows, w_o, preferred_element_type=jnp.float32) + b_o).astype(jnp.bfloat16)
    normed2 = layer_norm(resid_rows, ln2_scale, ln2_shift)
    pre_act = jnp.dot(normed2, w_in, preferred_element_type=jnp.float32) + b_in
    hidden = jax.nn.gelu(pre_act, approximate=True).astype(jnp.bfloat16)
    out_rows = (resid_rows.astype(jnp.float32) + jnp.dot(hidden, w_out, preferred_element_type=jnp.float32) + b_out).astype(jnp.bfloat16)
    return out_rows.reshape(BATCH, SEQ_LEN, D_MODEL)


def reference(x_in, ln1_scale, ln1_shift, w_qkv, b_qkv, w_o, b_o, ln2_scale, ln2_shift, w_in, b_in, w_out, b_out, grad_out):
    out_val, pullback = jax.vjp(layer_forward, x_in, ln1_scale, ln1_shift, w_qkv, b_qkv, w_o, b_o, ln2_scale, ln2_shift, w_in, b_in, w_out, b_out)
    grads = pullback(grad_out)
    return (out_val, grads[0], grads[1], grads[2], grads[3], grads[4], grads[5], grads[6], grads[7], grads[8], grads[9], grads[10], grads[11], grads[12])
```

```python
import functools

import jax
import jax.numpy as jnp
from jax import lax
from jax.experimental import pallas as pl
from jax.experimental.pallas import tpu as pltpu
from jax.sharding import PartitionSpec as P

LN_EPS = 1e-5
LANES = 128
Q_BLOCK = 256
BF16 = jnp.bfloat16
F32 = jnp.float32


def gelu_tanh(pre_act):
    return jax.nn.gelu(pre_act, approximate=True)


def dot(lhs, rhs):
    return jnp.dot(lhs, rhs, preferred_element_type=F32)


def dot_tr(lhs, rhs):
    return lax.dot_general(lhs, rhs, (((1,), (1,)), ((), ())), preferred_element_type=F32)


def dot_tl(lhs, rhs):
    return lax.dot_general(lhs, rhs, (((0,), (0,)), ((), ())), preferred_element_type=F32)


def attn_fwd_kernel(scale, blk, q_ref, k_ref, v_ref, o_ref, m_ref, r_ref):
    seq_len = q_ref.shape[0]
    vals_t = v_ref[...].astype(F32).T.astype(BF16)
    key_pos = lax.broadcasted_iota(jnp.int32, (blk, blk), 0)
    query_pos = lax.broadcasted_iota(jnp.int32, (blk, blk), 1)
    keep = key_pos <= query_pos
    for start in range(0, seq_len, blk):
        rows = pl.ds(start, blk)
        query = q_ref[rows, :]
        diag = jnp.where(keep, dot_tr(k_ref[rows, :], query) * scale, -1e30)
        top = jnp.max(diag, axis=0, keepdims=True)
        if start:
            past = dot_tr(k_ref[pl.ds(0, start), :], query) * scale
            top = jnp.maximum(top, jnp.max(past, axis=0, keepdims=True))
            past = jnp.exp(past - top)
        diag = jnp.exp(diag - top)
        total = jnp.sum(diag, axis=0, keepdims=True)
        if start:
            total = total + jnp.sum(past, axis=0, keepdims=True)
        recip = 1.0 / total
        out_t = dot(vals_t[:, start:start + blk], (diag * recip).astype(BF16))
        if start:
            out_t = out_t + dot(vals_t[:, :start], (past * recip).astype(BF16))
        o_ref[rows, :] = out_t.T.astype(BF16)
        m_ref[0, :, rows] = top
        r_ref[0, :, rows] = recip


def attn_bwd_kernel(scale, blk, q_ref, k_ref, v_ref, do_ref, m_ref, r_ref, dq_ref, dk_ref, dv_ref, dk_acc, dv_acc):
    seq_len = q_ref.shape[0]
    keys_t = k_ref[...].astype(F32).T.astype(BF16)
    key_pos = lax.broadcasted_iota(jnp.int32, (blk, blk), 0)
    query_pos = lax.broadcasted_iota(jnp.int32, (blk, blk), 1)
    keep = key_pos <= query_pos
    dk_acc[...] = jnp.zeros_like(dk_acc)
    dv_acc[...] = jnp.zeros_like(dv_acc)
    for start in range(0, seq_len, blk):
        rows = pl.ds(start, blk)
        query, grad = q_ref[rows, :], do_ref[rows, :]
        top, recip = m_ref[0, :, rows], r_ref[0, :, rows]

        def probs_of(span, masked):
            scores = dot_tr(k_ref[span, :], query) * scale
            if masked:
                scores = jnp.where(keep, scores, -1e30)
            probs = jnp.exp(scores - top) * recip
            dv_acc[span, :] += dot(probs.astype(BF16), grad)
            gprobs = dot_tr(v_ref[span, :], grad)
            return probs, gprobs, jnp.sum(probs * gprobs, axis=0, keepdims=True)

        spans = [(rows, True, start, start + blk)]
        if start:
            spans.append((pl.ds(0, start), False, 0, start))
        parts = [probs_of(span, masked) for span, masked, _, _ in spans]
        delta = parts[0][2]
        if start:
            delta = delta + parts[1][2]
        dq_t = None
        for (span, _, lo, hi), (probs, gprobs, _) in zip(spans, parts):
            gscores = (probs * (gprobs - delta) * scale).astype(BF16)
            dk_acc[span, :] += dot(gscores, query)
            term = dot(keys_t[:, lo:hi], gscores)
            dq_t = term if dq_t is None else dq_t + term
        dq_ref[rows, :] = dq_t.T.astype(BF16)
    dk_ref[...] = dk_acc[...].astype(BF16)
    dv_ref[...] = dv_acc[...].astype(BF16)


def attn_specs(seq_len, part):
    return pl.BlockSpec((seq_len, LANES), lambda i, h: (i, 3 * h + part))


def attention_fwd(qkv_pad, seq_count, heads, head_dim):
    seq_len = qkv_pad.shape[0] // seq_count
    items = seq_count * heads
    head_spec = pl.BlockSpec((seq_len, LANES), lambda i, h: (i, h))
    stat_spec = pl.BlockSpec((1, 1, seq_len), lambda i, h: (i * heads + h, 0, 0))
    flops = items * 4 * seq_len * seq_len * LANES // 2
    return pl.pallas_call(
        functools.partial(attn_fwd_kernel, head_dim ** -0.5, min(Q_BLOCK, seq_len)),
        grid=(seq_count, heads),
        in_specs=[attn_specs(seq_len, part) for part in range(3)],
        out_specs=[head_spec, stat_spec, stat_spec],
        out_shape=[jax.ShapeDtypeStruct((qkv_pad.shape[0], heads * LANES), BF16)] + [jax.ShapeDtypeStruct((items, 1, seq_len), F32)] * 2,
        cost_estimate=pl.CostEstimate(flops=8 * flops, bytes_accessed=qkv_pad.size * 3, transcendentals=0),
        compiler_params=pltpu.CompilerParams(vmem_limit_bytes=48 << 20),
        name="attn_fwd",
    )(qkv_pad, qkv_pad, qkv_pad)


def attention_bwd(qkv_pad, grad_pad, tops, recips, seq_count, heads, head_dim):
    seq_len = qkv_pad.shape[0] // seq_count
    items = seq_count * heads
    head_spec = pl.BlockSpec((seq_len, LANES), lambda i, h: (i, h))
    stat_spec = pl.BlockSpec((1, 1, seq_len), lambda i, h: (i * heads + h, 0, 0))
    flops = items * 10 * seq_len * seq_len * LANES // 2
    return pl.pallas_call(
        functools.partial(attn_bwd_kernel, head_dim ** -0.5, min(Q_BLOCK, seq_len)),
        grid=(seq_count, heads),
        in_specs=[attn_specs(seq_len, part) for part in range(3)] + [head_spec, stat_spec, stat_spec],
        out_specs=[head_spec] * 3,
        out_shape=[jax.ShapeDtypeStruct((qkv_pad.shape[0], heads * LANES), BF16)] * 3,
        scratch_shapes=[pltpu.VMEM((seq_len, LANES), F32)] * 2,
        cost_estimate=pl.CostEstimate(flops=8 * flops, bytes_accessed=qkv_pad.size * 4, transcendentals=0),
        compiler_params=pltpu.CompilerParams(vmem_limit_bytes=48 << 20),
        name="attn_bwd",
    )(qkv_pad, qkv_pad, qkv_pad, grad_pad, tops, recips)


def pad_heads(arr, heads, head_dim):
    lead = arr.shape[:-1]
    arr = arr.reshape(lead + (heads, head_dim))
    arr = jnp.pad(arr, [(0, 0)] * (len(lead) + 1) + [(0, LANES - head_dim)])
    return arr.reshape(lead + (heads * LANES,))


def unpad_heads(arr, heads, head_dim):
    lead = arr.shape[:-1]
    return arr.reshape(lead + (heads, LANES))[..., :head_dim].reshape(lead + (heads * head_dim,))


def norm_rows(act_f32):
    mean_val = jnp.mean(act_f32, axis=-1, keepdims=True)
    variance = jnp.mean(act_f32 * act_f32, axis=-1, keepdims=True) - mean_val * mean_val
    inv_std = lax.rsqrt(variance + LN_EPS)
    return (act_f32 - mean_val) * inv_std, inv_std


def layer_norm(act_in, ln_scale, ln_shift):
    return (norm_rows(act_in.astype(F32))[0] * ln_scale + ln_shift).astype(BF16)


def layer_norm_bwd(grad_bf16, act_in, ln_scale):
    grad_f32 = grad_bf16.astype(F32)
    normed, inv_std = norm_rows(act_in.astype(F32))
    grad_hat = grad_f32 * ln_scale
    mean_a = jnp.mean(grad_hat, axis=-1, keepdims=True)
    mean_b = jnp.mean(grad_hat * normed, axis=-1, keepdims=True)
    grad_in = inv_std * (grad_hat - mean_a - normed * mean_b)
    return grad_in, jnp.sum(grad_f32 * normed, axis=0), jnp.sum(grad_f32, axis=0)


def ring_gather(blk, size, axis):
    me = lax.axis_index('col')
    width = blk.shape[axis]
    up = [(i, (i + 1) % size) for i in range(size)]
    down = [(i, (i - 1) % size) for i in range(size)]
    half = blk.shape[0] // 2
    whole_shape = list(blk.shape)
    whole_shape[axis] = width * size

    def place(whole, part, owner, row_off):
        offs = [0] * blk.ndim
        offs[0] = row_off
        offs[axis] = offs[axis] + lax.rem(owner + 2 * size, size) * width
        return lax.dynamic_update_slice(whole, part, tuple(offs))

    whole = place(jnp.zeros(tuple(whole_shape), blk.dtype), blk, me, 0)
    from_low = lax.ppermute(blk, 'col', up)
    from_high = lax.ppermute(blk, 'col', down)
    far_a = lax.ppermute(from_low[:half], 'col', up)
    far_b = lax.ppermute(from_high[half:], 'col', down)
    whole = place(whole, from_low, me - 1, 0)
    whole = place(whole, from_high, me + 1, 0)
    whole = place(whole, far_a, me + 2, 0)
    return place(whole, far_b, me + 2, half)


def tie(value, *others):
    return lax.optimization_barrier((value, *others))


def ring_scatter(part, size, axis, between=None):
    me = lax.axis_index('col')
    width = part.shape[axis] // size
    up = [(i, (i + 1) % size) for i in range(size)]
    down = [(i, (i - 1) % size) for i in range(size)]

    def block(owner):
        return lax.dynamic_slice_in_dim(part, lax.rem(owner + size, size) * width, width, axis)

    far, high, low, own = block(me + 2), block(me + 1), block(me - 1), block(me)
    half = own.shape[0] // 2
    from_low = lax.ppermute(far[:half], 'col', up)
    from_high = lax.ppermute(far[half:], 'col', down)
    if between is not None:
        from_low, from_high = between(from_low, from_high)
    got_a = lax.ppermute(jnp.concatenate([high[:half] + from_low, high[half:]], axis=0), 'col', up)
    got_b = lax.ppermute(jnp.concatenate([low[:half], low[half:] + from_high], axis=0), 'col', down)
    return own + got_a + got_b


def exchange(arr, size, split_axis, join_axis):
    me = lax.axis_index('col')
    width = arr.shape[split_axis] // size
    shape = list(arr.shape)
    shape[split_axis] = width
    join = shape[join_axis]
    shape[join_axis] = join * size
    whole = jnp.zeros(tuple(shape), arr.dtype)
    for shift in range(size):
        target = lax.rem(me + shift, size)
        part = lax.dynamic_slice_in_dim(arr, target * width, width, split_axis)
        if shift:
            part = lax.ppermute(part, 'col', [(i, (i + shift) % size) for i in range(size)])
        source = lax.rem(me + size - shift, size)
        whole = lax.dynamic_update_slice_in_dim(whole, part, source * join, join_axis)
    return whole


def solution(mesh):
    cols = mesh.shape['col']
    rows = mesh.shape['row']
    per = rows // cols
    assert cols == 4 and rows == cols * per
    act_spec = P(('dp', 'row'), None, 'col')
    vec_spec = P('col')
    mat_spec = P('row', 'col')
    head_spec = P('col', None)
    gvec_spec = P(('dp', 'col'))
    gmat_spec = P(('dp', 'row'), 'col')
    ghead_spec = P(('dp', 'col'), None)
    flip = [(b * rows + a * per + k, a * rows + b * per + k) for a in range(cols) for k in range(per) for b in range(cols)]

    def gather_rows(w_blk):
        return lax.all_gather(w_blk, 'row', axis=0, tiled=True)

    def gather_vec(vec):
        return lax.all_gather(vec, 'col', axis=0, tiled=True)

    def scatter_rows(part):
        return lax.psum_scatter(part, 'row', scatter_dimension=0, tiled=True)

    def row_split_weight(w_blk):
        depth, width = w_blk.shape
        moved = lax.ppermute(w_blk, ('col', 'row'), flip)
        stack = gather_rows(moved).reshape(cols, per, depth, width)
        return stack.transpose(1, 2, 0, 3).reshape(per * depth, cols * width)

    def row_split_part(lhs, rhs):
        width = rhs.shape[1] // cols
        depth = lhs.shape[1] // per
        part = jnp.concatenate([dot_tl(lhs, rhs[:, j * width:(j + 1) * width]) for j in range(cols)], axis=0)
        return part.reshape(rows * depth, width)

    def to_owner(block):
        return lax.ppermute(block.astype(BF16), ('col', 'row'), flip)

    def layer_block(x_blk, ln1_scale, ln1_shift, w_qkv, b_qkv, w_o, b_o, ln2_scale, ln2_shift, w_in, b_in, w_out, b_out, grad_blk):
        seq_count, seq_len, d_local = x_blk.shape
        tokens = seq_count * seq_len
        tok_local = tokens // cols
        heads, qkv_width = b_qkv.shape
        head_dim = qkv_width // 3
        me = lax.axis_index('col')
        x_loc = x_blk.reshape(tokens, d_local)
        g_loc = grad_blk.reshape(tokens, d_local)

        def own_tokens(arr):
            return lax.dynamic_slice_in_dim(arr, me * tok_local, tok_local, 0)

        def own_feats(arr):
            return lax.dynamic_slice_in_dim(arr, me * d_local, d_local, arr.ndim - 1)

        vecs = gather_vec(jnp.stack([ln1_scale, ln1_shift, ln2_scale, ln2_shift, b_o], axis=1))
        scale1, shift1, scale2, shift2, bias_o = [vecs[:, i] for i in range(5)]

        x_full = ring_gather(x_loc, cols, 1)
        w_qkv_full = gather_rows(w_qkv)
        w_out_blk, w_o_blk, w_in_blk, g_blk, x_full = lax.optimization_barrier((w_out, w_o, w_in, g_loc, x_full))
        w_o_full = ring_gather(gather_rows(w_o_blk), cols, 1)
        w_out_rows = row_split_weight(w_out_blk)
        w_in_full = gather_rows(w_in_blk)
        g_full = ring_gather(g_blk, cols, 1)

        normed1 = layer_norm(x_full, scale1, shift1)
        w_qkv_pad = pad_heads(w_qkv_full, 3 * heads, head_dim)
        b_qkv_pad = pad_heads(b_qkv.reshape(heads * qkv_width), 3 * heads, head_dim)
        qkv_pad = (dot(normed1, w_qkv_pad) + b_qkv_pad).astype(BF16)
        o_pad, tops, recips = attention_fwd(qkv_pad, seq_count, heads, head_dim)
        o_loc = unpad_heads(o_pad, heads, head_dim)
        o_tok = exchange(o_loc, cols, 0, 1)
        r1_tok = (own_tokens(x_full).astype(F32) + dot(o_tok, w_o_full) + bias_o).astype(BF16)
        grad_hidden = dot_tr(g_full, w_out_rows).astype(BF16)
        r1_full = ring_gather(r1_tok, cols, 0)
        normed2 = layer_norm(r1_full, scale2, shift2)
        pre_act = dot(normed2, w_in_full) + b_in
        hidden, gelu_back = jax.vjp(gelu_tanh, pre_act)
        hidden = hidden.astype(BF16)
        grad_pre = gelu_back(grad_hidden.astype(F32))[0]
        grad_pre_bf = grad_pre.astype(BF16)

        gh2 = ring_scatter(dot_tr(grad_pre_bf, w_in_full), cols, 0).astype(BF16)
        gh2, part_w_out, out_part = tie(gh2, row_split_part(hidden, g_full), dot(hidden, w_out_rows))
        ln2_grad, ln2_gscale, ln2_gshift = layer_norm_bwd(gh2, r1_tok, scale2)
        gr1_tok = (own_tokens(g_full).astype(F32) + ln2_grad).astype(BF16)
        gr1_full = ring_gather(gr1_tok, cols, 0)
        gr1_full, part_w_in, out_part = tie(gr1_full, dot_tl(normed2, grad_pre_bf), out_part)
        w_o_pad = pad_heads(lax.dynamic_slice_in_dim(w_o_full, me * d_local, d_local, 0).T, heads, head_dim)
        grad_o_pad = dot(gr1_full, w_o_pad).astype(BF16)
        grad_o_pad, sum_w_out = tie(grad_o_pad, scatter_rows(part_w_out))
        dq, dk, dv = attention_bwd(qkv_pad, grad_o_pad, tops, recips, seq_count, heads, head_dim)
        grads = [a.reshape(tokens, heads, LANES)[..., :head_dim] for a in (dq, dk, dv)]
        grad_qkv = jnp.stack(grads, axis=2).reshape(tokens, heads * qkv_width)

        def under_attention(from_low, from_high):
            nonlocal grad_qkv
            grad_qkv, from_low, from_high = tie(grad_qkv, from_low, from_high)
            return from_low, from_high

        out_sum = ring_scatter(out_part, cols, 1, under_attention)
        out_rows = (own_feats(r1_full).astype(F32) + out_sum + b_out).astype(BF16)
        gh1 = ring_scatter(dot_tr(grad_qkv, w_qkv_full), cols, 0).astype(BF16)
        gh1, part_w_o, part_w_qkv, sum_w_in = tie(gh1, row_split_part(o_loc, gr1_full), dot_tl(normed1, grad_qkv), scatter_rows(part_w_in))
        ln1_grad, ln1_gscale, ln1_gshift = layer_norm_bwd(gh1, own_tokens(x_full), scale1)
        gx_tok = (gr1_tok.astype(F32) + ln1_grad).astype(BF16)
        grad_x = exchange(gx_tok, cols, 1, 0)

        grad_w_out = to_owner(sum_w_out)
        grad_w_in = sum_w_in.astype(BF16)
        grad_w_o = to_owner(scatter_rows(part_w_o))
        grad_w_qkv = scatter_rows(part_w_qkv).astype(BF16)

        def tok_sum(arr):
            return jnp.sum(arr.astype(F32), axis=0)

        early = lax.psum(jnp.concatenate([tok_sum(grad_pre), tok_sum(g_loc), tok_sum(own_feats(gr1_full)), tok_sum(grad_qkv)]), 'row')
        ff_local = b_in.shape[0]
        gb_in, gb_out, gb_o, gb_qkv = jnp.split(early, [ff_local, ff_local + d_local, ff_local + 2 * d_local])
        late = lax.psum(jnp.stack([ln1_gscale, ln1_gshift, ln2_gscale, ln2_gshift]), ('col', 'row'))
        g_ln = own_feats(late)
        return (out_rows.reshape(x_blk.shape), grad_x.reshape(x_blk.shape), g_ln[0], g_ln[1], grad_w_qkv, gb_qkv.reshape(heads, qkv_width), grad_w_o, gb_o, g_ln[2], g_ln[3], grad_w_in, gb_in, grad_w_out, gb_out)

    return jax.shard_map(layer_block, mesh=mesh,
                         in_specs=(act_spec, vec_spec, vec_spec, mat_spec, head_spec, mat_spec, vec_spec, vec_spec, vec_spec, mat_spec, vec_spec, mat_spec, vec_spec, act_spec),
                         out_specs=(act_spec, act_spec, gvec_spec, gvec_spec, gmat_spec, ghead_spec, gmat_spec, gvec_spec, gvec_spec, gvec_spec, gmat_spec, gvec_spec, gmat_spec, gvec_spec),
                         check_vma=False)
```

```python
import functools

import jax
import jax.numpy as jnp
from jax import lax
from jax.experimental import pallas as pl
from jax.experimental.pallas import tpu as pltpu
from jax.sharding import PartitionSpec as P

LN_EPS = 1e-5
LANES = 128
Q_BLOCK = 256
BF16 = jnp.bfloat16
F32 = jnp.float32


def gelu_tanh(pre_act):
    return jax.nn.gelu(pre_act, approximate=True)


def dot(lhs, rhs):
    return jnp.dot(lhs, rhs, preferred_element_type=F32)


def dot_tr(lhs, rhs):
    return lax.dot_general(lhs, rhs, (((1,), (1,)), ((), ())), preferred_element_type=F32)


def dot_tl(lhs, rhs):
    return lax.dot_general(lhs, rhs, (((0,), (0,)), ((), ())), preferred_element_type=F32)


def attn_fwd_kernel(scale, blk, q_ref, k_ref, v_ref, o_ref, m_ref, r_ref):
    seq_len = q_ref.shape[0]
    vals_t = v_ref[...].astype(F32).T.astype(BF16)
    key_pos = lax.broadcasted_iota(jnp.int32, (blk, blk), 0)
    query_pos = lax.broadcasted_iota(jnp.int32, (blk, blk), 1)
    keep = key_pos <= query_pos
    for start in range(0, seq_len, blk):
        rows = pl.ds(start, blk)
        query = q_ref[rows, :]
        diag = jnp.where(keep, dot_tr(k_ref[rows, :], query) * scale, -1e30)
        top = jnp.max(diag, axis=0, keepdims=True)
        if start:
            past = dot_tr(k_ref[pl.ds(0, start), :], query) * scale
            top = jnp.maximum(top, jnp.max(past, axis=0, keepdims=True))
            past = jnp.exp(past - top)
        diag = jnp.exp(diag - top)
        total = jnp.sum(diag, axis=0, keepdims=True)
        if start:
            total = total + jnp.sum(past, axis=0, keepdims=True)
        recip = 1.0 / total
        out_t = dot(vals_t[:, start:start + blk], (diag * recip).astype(BF16))
        if start:
            out_t = out_t + dot(vals_t[:, :start], (past * recip).astype(BF16))
        o_ref[rows, :] = out_t.T.astype(BF16)
        m_ref[0, :, rows] = top
        r_ref[0, :, rows] = recip


def attn_bwd_kernel(scale, blk, q_ref, k_ref, v_ref, do_ref, m_ref, r_ref, *rest):
    grad_ref, dk_acc, dv_acc = rest[-3:]
    seq_len = q_ref.shape[0]
    keys_t = k_ref[...].astype(F32).T.astype(BF16)
    key_pos = lax.broadcasted_iota(jnp.int32, (blk, blk), 0)
    query_pos = lax.broadcasted_iota(jnp.int32, (blk, blk), 1)
    keep = key_pos <= query_pos
    dk_acc[...] = jnp.zeros_like(dk_acc)
    dv_acc[...] = jnp.zeros_like(dv_acc)
    for start in range(0, seq_len, blk):
        rows = pl.ds(start, blk)
        query, grad = q_ref[rows, :], do_ref[rows, :]
        top, recip = m_ref[0, :, rows], r_ref[0, :, rows]

        def probs_of(span, masked):
            scores = dot_tr(k_ref[span, :], query) * scale
            if masked:
                scores = jnp.where(keep, scores, -1e30)
            probs = jnp.exp(scores - top) * recip
            dv_acc[span, :] += dot(probs.astype(BF16), grad)
            gprobs = dot_tr(v_ref[span, :], grad)
            return probs, gprobs, jnp.sum(probs * gprobs, axis=0, keepdims=True)

        spans = [(rows, True, start, start + blk)]
        if start:
            spans.append((pl.ds(0, start), False, 0, start))
        parts = [probs_of(span, masked) for span, masked, _, _ in spans]
        delta = parts[0][2]
        if start:
            delta = delta + parts[1][2]
        dq_t = None
        for (span, _, lo, hi), (probs, gprobs, _) in zip(spans, parts):
            gscores = (probs * (gprobs - delta) * scale).astype(BF16)
            dk_acc[span, :] += dot(gscores, query)
            term = dot(keys_t[:, lo:hi], gscores)
            dq_t = term if dq_t is None else dq_t + term
        grad_ref[rows, 0:LANES] = dq_t.T.astype(BF16)
    grad_ref[:, LANES:2 * LANES] = dk_acc[...].astype(BF16)
    grad_ref[:, 2 * LANES:] = dv_acc[...].astype(BF16)


def attn_specs(seq_len, part):
    return pl.BlockSpec((seq_len, LANES), lambda i, h: (i, 3 * h + part))


def attention_fwd(qkv_pad, seq_count, heads, head_dim):
    seq_len = qkv_pad.shape[0] // seq_count
    items = seq_count * heads
    head_spec = pl.BlockSpec((seq_len, LANES), lambda i, h: (i, h))
    stat_spec = pl.BlockSpec((1, 1, seq_len), lambda i, h: (i * heads + h, 0, 0))
    flops = items * 4 * seq_len * seq_len * LANES // 2
    return pl.pallas_call(
        functools.partial(attn_fwd_kernel, head_dim ** -0.5, min(Q_BLOCK, seq_len)),
        grid=(seq_count, heads),
        in_specs=[attn_specs(seq_len, part) for part in range(3)],
        out_specs=[head_spec, stat_spec, stat_spec],
        out_shape=[jax.ShapeDtypeStruct((qkv_pad.shape[0], heads * LANES), BF16)] + [jax.ShapeDtypeStruct((items, 1, seq_len), F32)] * 2,
        cost_estimate=pl.CostEstimate(flops=8 * flops, bytes_accessed=qkv_pad.size * 3, transcendentals=0),
        compiler_params=pltpu.CompilerParams(vmem_limit_bytes=48 << 20),
        name="attn_fwd",
    )(qkv_pad, qkv_pad, qkv_pad)


def attention_bwd(qkv_pad, grad_pad, tops, recips, seq_count, heads, head_dim, first, count, partial=None):
    seq_len = qkv_pad.shape[0] // seq_count
    stat_spec = pl.BlockSpec((1, 1, seq_len), lambda i, h: (i * heads + first + h, 0, 0))
    in_specs = [pl.BlockSpec((seq_len, LANES), lambda i, h, part=part: (i, 3 * (first + h) + part)) for part in range(3)]
    in_specs += [pl.BlockSpec((seq_len, LANES), lambda i, h: (i, first + h)), stat_spec, stat_spec]
    operands = [qkv_pad, qkv_pad, qkv_pad, grad_pad, tops, recips]
    aliases = {}
    if partial is not None:
        aliases = {len(operands): 0}
        in_specs.append(pl.BlockSpec(memory_space=pl.ANY))
        operands.append(partial)
    flops = seq_count * count * 10 * seq_len * seq_len * LANES // 2
    return pl.pallas_call(
        functools.partial(attn_bwd_kernel, head_dim ** -0.5, min(Q_BLOCK, seq_len)),
        grid=(seq_count, count),
        in_specs=in_specs,
        out_specs=pl.BlockSpec((seq_len, 3 * LANES), lambda i, h: (i, first + h)),
        out_shape=jax.ShapeDtypeStruct(qkv_pad.shape, BF16),
        scratch_shapes=[pltpu.VMEM((seq_len, LANES), F32)] * 2,
        input_output_aliases=aliases,
        cost_estimate=pl.CostEstimate(flops=8 * flops, bytes_accessed=qkv_pad.size * 2, transcendentals=0),
        compiler_params=pltpu.CompilerParams(vmem_limit_bytes=48 << 20),
        name="attn_bwd",
    )(*operands)


def pad_heads(arr, heads, head_dim):
    lead = arr.shape[:-1]
    arr = arr.reshape(lead + (heads, head_dim))
    arr = jnp.pad(arr, [(0, 0)] * (len(lead) + 1) + [(0, LANES - head_dim)])
    return arr.reshape(lead + (heads * LANES,))


def unpad_heads(arr, heads, head_dim):
    lead = arr.shape[:-1]
    return arr.reshape(lead + (heads, LANES))[..., :head_dim].reshape(lead + (heads * head_dim,))


def norm_rows(act_f32):
    mean_val = jnp.mean(act_f32, axis=-1, keepdims=True)
    variance = jnp.mean(act_f32 * act_f32, axis=-1, keepdims=True) - mean_val * mean_val
    inv_std = lax.rsqrt(variance + LN_EPS)
    return (act_f32 - mean_val) * inv_std, inv_std


def layer_norm(act_in, ln_scale, ln_shift):
    return (norm_rows(act_in.astype(F32))[0] * ln_scale + ln_shift).astype(BF16)


def layer_norm_bwd(grad_bf16, act_in, ln_scale):
    grad_f32 = grad_bf16.astype(F32)
    normed, inv_std = norm_rows(act_in.astype(F32))
    grad_hat = grad_f32 * ln_scale
    mean_a = jnp.mean(grad_hat, axis=-1, keepdims=True)
    mean_b = jnp.mean(grad_hat * normed, axis=-1, keepdims=True)
    grad_in = inv_std * (grad_hat - mean_a - normed * mean_b)
    return grad_in, jnp.sum(grad_f32 * normed, axis=0), jnp.sum(grad_f32, axis=0)


def ring_gather(blk, size, axis, between=None, after=None):
    me = lax.axis_index('col')
    width = blk.shape[axis]
    up = [(i, (i + 1) % size) for i in range(size)]
    down = [(i, (i - 1) % size) for i in range(size)]
    half = blk.shape[0] // 2
    whole_shape = list(blk.shape)
    whole_shape[axis] = width * size

    def place(whole, part, owner, row_off):
        offs = [0] * blk.ndim
        offs[0] = row_off
        offs[axis] = offs[axis] + lax.rem(owner + 2 * size, size) * width
        return lax.dynamic_update_slice(whole, part, tuple(offs))

    whole = place(jnp.zeros(tuple(whole_shape), blk.dtype), blk, me, 0)
    from_low = lax.ppermute(blk, 'col', up)
    from_high = lax.ppermute(blk, 'col', down)
    if between is not None:
        from_low, from_high = between(from_low, from_high)
    far_a = lax.ppermute(from_low[:half], 'col', up)
    far_b = lax.ppermute(from_high[half:], 'col', down)
    if after is not None:
        far_a, far_b = after(far_a, far_b)
    whole = place(whole, from_low, me - 1, 0)
    whole = place(whole, from_high, me + 1, 0)
    whole = place(whole, far_a, me + 2, 0)
    return place(whole, far_b, me + 2, half)


def tie(value, *others):
    return lax.optimization_barrier((value, *others))


def ring_scatter(part, size, axis, between=None):
    me = lax.axis_index('col')
    width = part.shape[axis] // size
    up = [(i, (i + 1) % size) for i in range(size)]
    down = [(i, (i - 1) % size) for i in range(size)]

    def block(owner):
        return lax.dynamic_slice_in_dim(part, lax.rem(owner + size, size) * width, width, axis)

    far, high, low, own = block(me + 2), block(me + 1), block(me - 1), block(me)
    half = own.shape[0] // 2
    from_low = lax.ppermute(far[:half], 'col', up)
    from_high = lax.ppermute(far[half:], 'col', down)
    if between is not None:
        from_low, from_high = between(from_low, from_high)
    got_a = lax.ppermute(jnp.concatenate([high[:half] + from_low, high[half:]], axis=0), 'col', up)
    got_b = lax.ppermute(jnp.concatenate([low[:half], low[half:] + from_high], axis=0), 'col', down)
    return own + got_a + got_b


def exchange(arr, size, split_axis, join_axis):
    me = lax.axis_index('col')
    width = arr.shape[split_axis] // size
    shape = list(arr.shape)
    shape[split_axis] = width
    join = shape[join_axis]
    shape[join_axis] = join * size
    whole = jnp.zeros(tuple(shape), arr.dtype)
    for shift in range(size):
        target = lax.rem(me + shift, size)
        part = lax.dynamic_slice_in_dim(arr, target * width, width, split_axis)
        if shift:
            part = lax.ppermute(part, 'col', [(i, (i + shift) % size) for i in range(size)])
        source = lax.rem(me + size - shift, size)
        whole = lax.dynamic_update_slice_in_dim(whole, part, source * join, join_axis)
    return whole


def solution(mesh):
    cols = mesh.shape['col']
    rows = mesh.shape['row']
    per = rows // cols
    assert cols == 4 and rows == cols * per
    act_spec = P(('dp', 'row'), None, 'col')
    vec_spec = P('col')
    mat_spec = P('row', 'col')
    head_spec = P('col', None)
    gvec_spec = P(('dp', 'col'))
    gmat_spec = P(('dp', 'row'), 'col')
    ghead_spec = P(('dp', 'col'), None)
    flip = [(b * rows + a * per + k, a * rows + b * per + k) for a in range(cols) for k in range(per) for b in range(cols)]

    def gather_rows(w_blk):
        return lax.all_gather(w_blk, 'row', axis=0, tiled=True)

    def scatter_rows(part):
        return lax.psum_scatter(part, 'row', scatter_dimension=0, tiled=True)

    def row_split_weight(w_blk):
        depth, width = w_blk.shape
        stack = gather_rows(w_blk).reshape(cols, per, depth, width)
        return stack.transpose(1, 2, 0, 3).reshape(per * depth, cols * width)

    def row_split_part(lhs, rhs):
        width = rhs.shape[1] // cols
        depth = lhs.shape[1] // per
        part = jnp.concatenate([dot_tl(lhs, rhs[:, j * width:(j + 1) * width]) for j in range(cols)], axis=0)
        return part.reshape(rows * depth, width)

    def to_owner(block):
        return lax.ppermute(block.astype(BF16), ('col', 'row'), flip)

    def layer_block(x_blk, ln1_scale, ln1_shift, w_qkv, b_qkv, w_o, b_o, ln2_scale, ln2_shift, w_in, b_in, w_out, b_out, grad_blk):
        seq_count, seq_len, d_local = x_blk.shape
        tokens = seq_count * seq_len
        tok_local = tokens // cols
        heads, qkv_width = b_qkv.shape
        head_dim = qkv_width // 3
        me = lax.axis_index('col')
        x_loc = x_blk.reshape(tokens, d_local)
        g_loc = grad_blk.reshape(tokens, d_local)

        def own_tokens(arr):
            return lax.dynamic_slice_in_dim(arr, me * tok_local, tok_local, 0)

        def own_feats(arr):
            return lax.dynamic_slice_in_dim(arr, me * d_local, d_local, arr.ndim - 1)

        w_out_moved = lax.ppermute(w_out, ('col', 'row'), flip)
        vecs = ring_gather(jnp.stack([ln1_scale, ln1_shift, ln2_scale, ln2_shift, b_o]), cols, 1)
        scale1, shift1, scale2, shift2, bias_o = [vecs[i] for i in range(5)]
        x_full = ring_gather(x_loc, cols, 1)
        w_qkv_full = gather_rows(w_qkv)
        w_o_cols = gather_rows(w_o)
        w_in_full = gather_rows(w_in)
        g_blk, w_out_moved, x_full = tie(g_loc, w_out_moved, x_full)
        w_out_rows = row_split_weight(w_out_moved)

        normed1 = layer_norm(x_full, scale1, shift1)
        w_qkv_pad = pad_heads(w_qkv_full, 3 * heads, head_dim)
        b_qkv_pad = pad_heads(b_qkv.reshape(heads * qkv_width), 3 * heads, head_dim)
        qkv_pad = (dot(normed1, w_qkv_pad) + b_qkv_pad).astype(BF16)

        def under_qkv(from_low, from_high):
            nonlocal qkv_pad, w_o_cols
            qkv_pad, w_o_cols, from_low, from_high = tie(qkv_pad, w_o_cols, from_low, from_high)
            return from_low, from_high

        def under_attention(far_a, far_b):
            nonlocal o_pad, tops, recips, w_o_full
            o_pad, tops, recips = attention_fwd(qkv_pad, seq_count, heads, head_dim)
            w_o_full = ring_gather(w_o_cols, cols, 1)
            o_pad, far_a, far_b = tie(o_pad, far_a, far_b)
            return far_a, far_b

        o_pad = tops = recips = w_o_full = None
        g_full = ring_gather(g_blk, cols, 1, under_qkv, under_attention)
        o_loc = unpad_heads(o_pad, heads, head_dim)
        o_tok = exchange(o_loc, cols, 0, 1)
        r1_tok = (own_tokens(x_full).astype(F32) + dot(o_tok, w_o_full) + bias_o).astype(BF16)
        grad_hidden = dot_tr(g_full, w_out_rows).astype(BF16)
        r1_full, grad_hidden = tie(ring_gather(r1_tok, cols, 0), grad_hidden)
        normed2 = layer_norm(r1_full, scale2, shift2)
        pre_act = dot(normed2, w_in_full) + b_in
        hidden, gelu_back = jax.vjp(gelu_tanh, pre_act)
        hidden = hidden.astype(BF16)
        grad_pre = gelu_back(grad_hidden.astype(F32))[0]
        grad_pre_bf = grad_pre.astype(BF16)

        gh2 = ring_scatter(dot_tr(grad_pre_bf, w_in_full), cols, 0).astype(BF16)
        part_w_out, out_part = row_split_part(hidden, g_full), dot(hidden, w_out_rows)
        gh2, part_w_out, out_part = tie(gh2, part_w_out, out_part)
        ln2_grad, ln2_gscale, ln2_gshift = layer_norm_bwd(gh2, r1_tok, scale2)
        gr1_tok = (own_tokens(g_full).astype(F32) + ln2_grad).astype(BF16)
        gr1_full = ring_gather(gr1_tok, cols, 0)
        part_w_in = dot_tl(normed2, grad_pre_bf)
        gr1_full, part_w_in, out_part = tie(gr1_full, part_w_in, out_part)
        w_o_pad = pad_heads(lax.dynamic_slice_in_dim(w_o_full, me * d_local, d_local, 0).T, heads, head_dim)
        grad_o_pad = dot(gr1_full, w_o_pad).astype(BF16)
        grad_o_pad, sum_w_out = tie(grad_o_pad, scatter_rows(part_w_out))
        part_w_o = row_split_part(tie(o_loc, grad_o_pad)[0], gr1_full)
        grad_o_pad = tie(grad_o_pad, part_w_o)[0]
        early_heads = max(heads // 2, 1)
        dqkv_pad = attention_bwd(qkv_pad, grad_o_pad, tops, recips, seq_count, heads, head_dim, 0, early_heads)

        def under_first_heads(from_low, from_high):
            nonlocal dqkv_pad
            dqkv_pad, from_low, from_high = tie(dqkv_pad, from_low, from_high)
            return from_low, from_high

        out_sum = ring_scatter(out_part, cols, 1, under_first_heads)
        if early_heads < heads:
            dqkv_pad = attention_bwd(qkv_pad, grad_o_pad, tops, recips, seq_count, heads, head_dim, early_heads, heads - early_heads, dqkv_pad)
        out_rows = (own_feats(r1_full).astype(F32) + out_sum + b_out).astype(BF16)
        grad_qkv = unpad_heads(dqkv_pad, 3 * heads, head_dim)
        gh1 = ring_scatter(dot_tr(dqkv_pad, w_qkv_pad), cols, 0).astype(BF16)
        part_w_qkv = dot_tl(normed1, grad_qkv)
        sum_w_in = scatter_rows(part_w_in)

        def tok_sum(arr):
            return jnp.sum(arr.astype(F32), axis=0)

        ff_local = b_in.shape[0]
        ln2_sums = ring_scatter(jnp.stack([ln2_gscale, ln2_gshift]), cols, 1)
        early = lax.psum(jnp.concatenate([tok_sum(grad_pre), tok_sum(g_loc), tok_sum(own_feats(gr1_full)), tok_sum(grad_qkv), ln2_sums[0], ln2_sums[1]]), 'row')
        gb_in, gb_out, gb_o, gb_qkv, g_ln2 = jnp.split(early, [ff_local, ff_local + d_local, ff_local + 2 * d_local, ff_local + 2 * d_local + heads * qkv_width])
        g_ln2 = g_ln2.reshape(2, d_local)

        gh1, part_w_qkv, _, _ = tie(gh1, part_w_qkv, sum_w_in, early)
        ln1_grad, ln1_gscale, ln1_gshift = layer_norm_bwd(gh1, own_tokens(x_full), scale1)
        gx_tok = (gr1_tok.astype(F32) + ln1_grad).astype(BF16)
        grad_x = exchange(gx_tok, cols, 1, 0)
        g_ln1 = lax.psum(ring_scatter(jnp.stack([ln1_gscale, ln1_gshift]), cols, 1), 'row')

        grad_w_out = to_owner(sum_w_out)
        grad_w_in = sum_w_in.astype(BF16)
        grad_w_o = to_owner(scatter_rows(part_w_o))
        grad_w_qkv = scatter_rows(part_w_qkv).astype(BF16)
        return (out_rows.reshape(x_blk.shape), grad_x.reshape(x_blk.shape), g_ln1[0], g_ln1[1], grad_w_qkv, gb_qkv.reshape(heads, qkv_width), grad_w_o, gb_o, g_ln2[0], g_ln2[1], grad_w_in, gb_in, grad_w_out, gb_out)

    return jax.shard_map(layer_block, mesh=mesh,
                         in_specs=(act_spec, vec_spec, vec_spec, mat_spec, head_spec, mat_spec, vec_spec, vec_spec, vec_spec, mat_spec, vec_spec, mat_spec, vec_spec, act_spec),
                         out_specs=(act_spec, act_spec, gvec_spec, gvec_spec, gmat_spec, ghead_spec, gmat_spec, gvec_spec, gvec_spec, gvec_spec, gmat_spec, gvec_spec, gmat_spec, gvec_spec),
                         check_vma=False)
```
